32 devices in a mesh: seq: 8 (over z, y), head: 4 (over x, core).
Axes of the slice: x: 2, y: 2, z: 4, core: 2. Of those that a mesh axis runs over, the one named last changes fastest.
Arguments:
- queries: bfloat16 [4096, 4096], P('seq', 'head'), may hold values from -5 to 5
- keys: bfloat16 [4096, 1024], P('seq', 'head'), may hold values from -5 to 5
- values: bfloat16 [4096, 1024], P('seq', 'head'), may hold values from -5 to 5
- doc_lengths: int32 [16], replicated, may hold values from 1 to 2048, 4096 in all
- out_weight: bfloat16 [4096, 4096], P('head', 'seq'), may hold values from -0.125 to 0.125
Outputs:
- mixed: bfloat16 [4096, 4096], P('seq', 'head')
The draws below stay inside these ranges and needn't reach their ends.
Inputs may be any that keep to these rules, and one draw needn't show every extreme that they name: `doc_lengths`: the lengths sum to 4096, and one document is exactly 2048 tokens long.
All inputs are finite; a program needn't handle non-finite values.
Results may differ from the reference program's by a relative error of at most 0.012.
Values may be sent and summed in bfloat16 or wider, within the bound.
No kernel may reach another device: no remote copies, remote signals or barrier semaphores. Data moves between devices by JAX's collectives and lax.ppermute only.
A program may use at most 128 MiB of HBM per device.

```python
import math
import jax
import jax.numpy as jnp
import numpy as np
from jax import lax

D = 4096
HQ = 32
KV = 8
DH = 128
TOK_DEV = 512
TOKENS = 4096
MOST = 2048
DOCS = 16


def draw_keys(key, part):
    base = jnp.clip(jax.random.normal(jax.random.fold_in(key, 1), (TOKENS, KV * DH), jnp.float32), -5.0, 5.0)
    return base.astype(jnp.bfloat16)


def draw_queries(key, part):
    base = jnp.clip(jax.random.normal(jax.random.fold_in(key, 2), (TOKENS, HQ * DH), jnp.float32), -5.0, 5.0)
    return base.astype(jnp.bfloat16)


def raised(array, key, source, target, parts, factor):
    def block_of(axis_at):
        return (jnp.arange(array.shape[axis_at]) // (array.shape[axis_at] // parts)).reshape((-1,) + (1,) * (array.ndim - 1 - axis_at))

    one_side = jax.random.permutation(key, parts)[block_of(target)]
    other_side = (block_of(target) + parts // 2) % parts
    return jnp.where((block_of(source) == one_side) | (block_of(source) == other_side), factor * array, array)


def steps_of(key, dims, cuts, low, high):
    gain, own = 1.0, jax.random.fold_in(key, 6)
    for axis_at, parts in cuts:
        heights = jnp.exp(jax.random.uniform(jax.random.fold_in(own, axis_at), (parts,), jnp.float32, low / len(cuts), high / len(cuts)))
        gain = gain * jnp.repeat(heights, dims[axis_at] // parts).reshape([-1 if axis == axis_at else 1 for axis in range(len(dims))])
    return gain


def length_profile(amount, total, most, slope):
    loads = [(1 << 20) // math.isqrt(grade ** slope) + 1 for grade in range(2, amount + 1)]
    rest, given = total - most - (amount - 1), [1] * (amount - 1)
    while rest > 0:
        free = [i for i in range(amount - 1) if given[i] < most]
        mass, left = sum([loads[i] for i in free]), rest
        for i in free:
            addition = min(most - given[i], max(1, left * loads[i] // mass), rest)
            given[i] = given[i] + addition
            rest = rest - addition
    return np.array([most] + given)


def uneven(stream_key, count, total, limit, slope):
    if count == 2:
        one = jax.random.randint(stream_key, (), max(1, total - limit), min(limit, total - 1) + 1)
        return jnp.stack([one, total - one])
    sizes = jnp.asarray(length_profile(count, total, limit, slope), jnp.int32)
    twos = (count - 1) // 2
    source_of, taker = sizes[1:1 + 2 * twos:2], sizes[2:2 + 2 * twos:2]
    margin = jnp.minimum(source_of - 1, limit - taker)
    passed = jax.random.randint(jax.random.fold_in(stream_key, 1), (twos,), 0, 1 << 20) % (margin + 1)
    sizes = sizes.at[1:1 + 2 * twos:2].set(source_of - passed).at[2:2 + 2 * twos:2].set(taker + passed)
    return sizes[jax.random.permutation(jax.random.fold_in(stream_key, 2), count)]


def normal_values(rng, dims, deviation, limit, split=(), kind=jnp.bfloat16):
    array = jax.random.normal(rng, dims, jnp.float32) * deviation
    if len(split) > 0:
        array = steps_of(rng, dims, split, -0.22, 0.18) * array
    return jnp.clip(array, min=-limit, max=limit).astype(kind)


def heavy_noise(stream_key, dims, width, bound, shards, heavy, held_as=jnp.bfloat16):
    entries = width * jax.random.normal(stream_key, dims, jnp.float32)
    if shards:
        entries = entries * steps_of(stream_key, dims, shards, -0.22, 0.18)
    return jnp.clip(raised(entries, jax.random.fold_in(stream_key, 3), *heavy), -bound, bound).astype(held_as)


def setup_inputs(seed: int = 0) -> dict:
    seeds = jax.random.split(jax.random.key(seed), 6)
    return {
        "queries": draw_queries(jax.random.fold_in(seeds[5], 71), 0),
        "keys": draw_keys(jax.random.fold_in(seeds[5], 71), 0),
        "values": normal_values(seeds[2], (TOKENS, KV * DH), 1.0, 5.0, ((0, 8), (1, 4))),
        "doc_lengths": uneven(seeds[3], DOCS, TOKENS, MOST, 2).astype(jnp.int32),
        "out_weight": heavy_noise(seeds[4], (HQ * DH, D), (HQ * DH) ** -0.5, 0.125, ((0, 4), (1, 8)), (0, 1, 8, 2.0)),
    }


def doc_index(positions, starts):
    return jnp.sum((starts[None, :] <= positions[:, None]).astype(jnp.int32), axis=1) - 1


def reference(queries, keys, values, doc_lengths, out_weight):
    starts = (jnp.cumsum(doc_lengths) - doc_lengths).astype(jnp.int32)
    total_rows = queries.shape[0]
    group_size = HQ // KV
    window = MOST + TOK_DEV
    num_blocks = total_rows // TOK_DEV
    temper = DH ** -0.5

    def attend_block(flat_index):
        q_block = flat_index // KV
        kv_head = flat_index % KV
        q_first = (q_block * TOK_DEV).astype(jnp.int32)
        k_first = jnp.clip(q_first - MOST, 0, total_rows - window).astype(jnp.int32)
        q_rows = lax.dynamic_slice(queries, (q_first, (kv_head * group_size * DH).astype(jnp.int32)), (TOK_DEV, group_size * DH))
        q_rows = q_rows.astype(jnp.float32).reshape(TOK_DEV, group_size, DH)
        k_rows = lax.dynamic_slice(keys, (k_first, (kv_head * DH).astype(jnp.int32)), (window, DH)).astype(jnp.float32)
        v_rows = lax.dynamic_slice(values, (k_first, (kv_head * DH).astype(jnp.int32)), (window, DH)).astype(jnp.float32)
        scores = jnp.einsum("qgd,nd->gqn", q_rows, k_rows) * temper
        q_pos = q_first + jnp.arange(TOK_DEV, dtype=jnp.int32)
        k_pos = k_first + jnp.arange(window, dtype=jnp.int32)
        q_doc = doc_index(q_pos, starts)
        k_doc = doc_index(k_pos, starts)
        allowed = (k_doc[None, :] == q_doc[:, None]) & (k_pos[None, :] <= q_pos[:, None])
        scores = jnp.where(allowed[None], scores, jnp.float32(-1e30))
        row_max = jnp.max(scores, axis=-1, keepdims=True)
        probs = jnp.where(allowed[None], jnp.exp(scores - row_max), jnp.float32(0.0))
        row_sum = jnp.sum(probs, axis=-1)
        weights = probs.astype(jnp.bfloat16)
        result = jnp.einsum("gqn,nd->gqd", weights.astype(jnp.float32), v_rows) / row_sum[..., None]
        return jnp.transpose(result, (1, 0, 2)).reshape(TOK_DEV, group_size * DH).astype(jnp.bfloat16)

    blocks = lax.map(attend_block, jnp.arange(num_blocks * KV, dtype=jnp.int32))
    attn = blocks.reshape(num_blocks, KV, TOK_DEV, group_size * DH)
    attn = jnp.transpose(attn, (0, 2, 1, 3)).reshape(total_rows, HQ * DH)
    return jnp.dot(attn, out_weight, preferred_element_type=jnp.float32).astype(jnp.bfloat16)
```

```python
import functools

import jax
import jax.numpy as jnp
import numpy as np
from jax import lax
from jax.experimental import pallas as pl
from jax.experimental.layout import Layout, with_layout_constraint
from jax.experimental.pallas import tpu as pltpu
from jax.sharding import PartitionSpec as P

HQ = 32
KV = 8
DH = 128
MOST = 2048
CALLS = 1


def attend_kernel(count, heads, column, first, lengths, q_ref, *refs):
    kv_refs = refs[: 2 * count]
    o_ref, k_buf, v_buf, m_ref, l_ref, acc_ref, sems = refs[2 * count + (not first) :]
    rows = q_ref.shape[0]
    factor = float(np.log2(np.e) / np.sqrt(DH))
    s, hops = lax.axis_index("seq"), count // 2 - 1
    q_first = s * rows

    def base_of(piece):
        hop = piece - hops - 1
        odd = s % 2
        along = s - 2 * piece
        across = jnp.where(odd == 1, s - 2 * hop - 1, s - 2 * hop + 1)
        valid = (across < s) & (hop <= hops - odd)
        return jnp.where(piece <= hops, along, jnp.where(valid, across, -(1 << 12))) * rows

    q_pos = q_first + lax.broadcasted_iota(jnp.int32, (1, rows), 1)

    def one_document(i, state):
        start, first_lo, last_lo, lo = state
        first_lo = jnp.where(start <= q_first, start, first_lo)
        last_lo = jnp.where(start < q_first + rows, start, last_lo)
        return start + lengths[i], first_lo, last_lo, jnp.where(start <= q_pos, start, lo)

    zero = jnp.int32(0)
    _, first_lo, last_lo, lo = lax.fori_loop(
        0, lengths.shape[0], one_document, (zero, zero, zero, jnp.zeros((1, rows), jnp.int32))
    )

    def copies(piece, at):
        for side, buf in enumerate((k_buf, v_buf)):
            yield pltpu.make_async_copy(
                kv_refs[side * count + at].at[:, column * DH : (column + 1) * DH],
                buf.at[piece],
                sems.at[side, piece],
            )

    for piece in range(count):

        @pl.when(first_lo < base_of(piece) + rows)
        def _():
            for copy in copies(piece, piece):
                copy.start()

    half = rows // 2

    def fold(piece, head, scores, first, columns):
        top = jnp.max(scores, axis=0, keepdims=True)
        if not first:
            old = m_ref[head, :, columns]
            top = jnp.maximum(old, top)
        probs = jnp.exp2((scores - top) * factor)
        total = jnp.sum(probs, axis=0, keepdims=True)
        out = lax.dot_general(
            v_buf[piece, : probs.shape[0]],
            probs.astype(jnp.bfloat16),
            (((0,), (0,)), ((), ())),
            preferred_element_type=jnp.float32,
        )
        if not first:
            fade = jnp.exp2((old - top) * factor)
            total = l_ref[head, :, columns] * fade + total
            out = acc_ref[head, :, columns] * fade + out
        m_ref[head, :, columns] = top
        l_ref[head, :, columns] = total
        acc_ref[head, :, columns] = out

    def scores_of(piece, head, count, columns):
        return lax.dot_general(
            k_buf[piece, :count],
            q_ref[columns, head * DH : (head + 1) * DH],
            (((1,), (1,)), ((), ())),
            preferred_element_type=jnp.float32,
        )

    for copy in copies(0, 0):
        copy.wait()
    for side in range(2):
        columns, deep = slice(side * half, (side + 1) * half), (side + 1) * half
        u = lax.broadcasted_iota(jnp.int32, (deep, half), 0)
        t = side * half + lax.broadcasted_iota(jnp.int32, (deep, half), 1)
        own = (u <= t) & (u >= lo[:, columns] - q_first)
        all_scores = [scores_of(0, head, deep, columns) for head in range(heads)]
        for head in range(heads):
            fold(0, head, jnp.where(own, all_scores[head], -1e30), True, columns)

    everything = slice(0, rows)

    @pl.loop(1, count)
    def _(piece):
        base = base_of(piece)
        needed = first_lo < base + rows

        @pl.when(needed)
        def _():
            for copy in copies(piece, 0):
                copy.wait()

        @pl.when(needed & (last_lo <= base))
        def _():
            all_scores = [scores_of(piece, head, rows, everything) for head in range(heads)]
            for head in range(heads):
                fold(piece, head, all_scores[head], False, everything)

        @pl.when(needed & (last_lo > base))
        def _():
            inside = lax.broadcasted_iota(jnp.int32, (rows, rows), 0) >= lo - base
            all_scores = [scores_of(piece, head, rows, everything) for head in range(heads)]
            for head in range(heads):
                fold(piece, head, jnp.where(inside, all_scores[head], -1e30), False, everything)

    for head in range(heads):
        result = acc_ref[head] / l_ref[head]
        o_ref[:, head * DH : (head + 1) * DH] = result.T.astype(jnp.bfloat16)


def attend(lengths, queries, ks, vs, call, group, attn):
    rows, count, first = queries.shape[0], len(ks), attn is None
    anywhere = pl.BlockSpec(memory_space=pl.ANY)
    return pl.pallas_call(
        functools.partial(attend_kernel, count, group, call // CALLS, first),
        grid=(1,),
        out_shape=jax.ShapeDtypeStruct(queries.shape, jnp.bfloat16),
        in_specs=[
            pl.BlockSpec(memory_space=pltpu.SMEM),
            pl.BlockSpec((rows, group * DH), lambda i: (0, call)),
        ]
        + [anywhere] * (2 * count + (not first)),
        out_specs=pl.BlockSpec((rows, group * DH), lambda i: (0, call)),
        scratch_shapes=[
            pltpu.VMEM((count, rows, DH), jnp.bfloat16),
            pltpu.VMEM((count, rows, DH), jnp.bfloat16),
            pltpu.VMEM((group, 1, rows), jnp.float32),
            pltpu.VMEM((group, 1, rows), jnp.float32),
            pltpu.VMEM((group, DH, rows), jnp.float32),
            pltpu.SemaphoreType.DMA((2, count)),
        ],
        input_output_aliases={} if first else {2 + 2 * count: 0},
        cost_estimate=pl.CostEstimate(
            flops=4 * rows * rows * DH * group * count,
            bytes_accessed=4 * rows * DH * (group + count),
            transcendentals=rows * rows * group * count,
        ),
    )(lengths, queries, *ks, *vs, *([] if first else [attn]))


def steps(queries, keys, values, doc_lengths, out_weight):
    n, nh = lax.axis_size("seq"), lax.axis_size("head")
    rows = queries.shape[0]
    kv_local = keys.shape[1] // DH
    hops = -(-(-(-MOST // rows)) // 2)
    blocks_per_head = n // nh
    s, h = lax.axis_index("seq"), lax.axis_index("head")

    def spread(own):
        same, across = [own], []
        for hop in range(hops + 1):
            if hop > 0:
                up = [(i - 2, i) for i in range(2 * hop, n)]
                same.append(lax.ppermute(same[-1], "seq", up))
            pairs = [(i ^ 1, i) for i in range(2 * hop, n)]
            if hop == 0:
                pairs = [p for p in pairs if p[1] % 2 == 1]
            elif hop == hops:
                pairs = [p for p in pairs if p[1] % 2 == 0]
            across.append(lax.ppermute(same[-1], "seq", pairs))
        return same + across

    ks, vs = spread(keys), spread(values)

    order = list(range(0, n, 2)) + list(range(n - 1, 0, -2))
    place = {v: i for i, v in enumerate(order)}
    ahead = [(order[i], order[(i + 1) % n]) for i in range(n)]
    behind = [(b, a) for a, b in ahead]
    depth, width = out_weight.shape
    blocks = {0: [out_weight[:, : width // 2], out_weight[:, width // 2 :]]}
    forth, back = list(blocks[0]), list(blocks[0])
    for i in range(1, n // 2):
        for part in range(2):
            forth[part] = lax.ppermute(forth[part], "seq", ahead)
            back[part] = lax.ppermute(back[part], "seq", behind)
        blocks[-i], blocks[i] = list(forth), list(back)
    upper, lower = slice(0, depth // 2), slice(depth // 2, depth)
    far = [
        [lax.ppermute(forth[0], "seq", ahead)],
        [lax.ppermute(forth[1][upper], "seq", ahead), lax.ppermute(back[1][lower], "seq", behind)],
    ]

    pairs_of = [(i, i - n // 2) for i in range(1, n // 2)]
    pairs_of.sort(key=lambda p: max(p[0], -p[1]))
    pairs_of.append((0, n // 2))
    final = len(pairs_of) - 1

    def goal(i, shift):
        return order[(place[i] + shift) % n]

    def place_of(block):
        return jnp.where(block % 2 == 0, block // 2, n // 2 + (n - 1 - block) // 2)

    def head_of(shift):
        at = (place_of(s) + shift + n) % n
        return jnp.where(at < n // 2, 2 * at, 2 * (n - 1 - at) + 1) // blocks_per_head

    attn = None
    for call in range(kv_local * CALLS):
        attn = attend(doc_lengths, queries, ks, vs, call, HQ // KV // CALLS, attn)

    def times(chosen):
        at, total = 0, None
        for w in chosen:
            term = jnp.dot(attn[:, at : at + w.shape[0]], w, preferred_element_type=jnp.float32)
            total = term if total is None else total + term
            at += w.shape[0]
        return total.astype(jnp.bfloat16)

    def added(one, two):
        return (one.astype(jnp.float32) + two.astype(jnp.float32)).astype(jnp.bfloat16)

    def reduced(step, ones, twos):
        one_first = ((head_of(pairs_of[step][0]) ^ h) & 1) == 1
        swap = [(i * nh + j, i * nh + (j ^ 1)) for i in range(n) for j in range(nh)]
        sent = [times([jnp.where(one_first, a, b) for a, b in zip(x, y)]) for x, y in zip(ones, twos)]
        part = jnp.concatenate(sent, axis=1)
        arrived = lax.ppermute(part, ("seq", "head"), swap)
        kept = [times([jnp.where(one_first, b, a) for a, b in zip(x, y)]) for x, y in zip(ones, twos)]
        part = added(jnp.concatenate(kept, axis=1), arrived)
        bit = 2
        while bit < nh:
            pairs = []
            for i in range(n):
                for j in range(nh):
                    for shift in pairs_of[step]:
                        off = j ^ (goal(i, shift) // blocks_per_head)
                        if off & bit and not off & (bit - 1):
                            pairs.append((i * nh + j, i * nh + (j ^ bit)))
            arrived = lax.ppermute(part, ("seq", "head"), pairs)
            bit *= 2
            if bit < nh:
                part = added(part, arrived)
        return added(part, arrived)

    def laid(array, step, column):
        rest = blocks_per_head * width - array.shape[1]
        total = None
        for slot in range(blocks_per_head):
            ahead_by = (place_of(h * blocks_per_head + slot) - place_of(s) + n) % n
            here = (ahead_by == pairs_of[step][0] % n) | (ahead_by == pairs_of[step][1] % n)
            begin = slot * width + column
            term = jnp.where(here, array, jnp.zeros_like(array))
            term = lax.pad(term, jnp.bfloat16(0), ((0, 0, 0), (begin, rest - begin, 0)))
            total = term if total is None else total + term
        return total

    mixed = None
    for step, (one, two) in enumerate(pairs_of[:-1]):
        whole = reduced(step, [[w] for w in blocks[one]], [[w] for w in blocks[two]])
        part = laid(whole, step, 0)
        mixed = part if mixed is None else mixed + part
    left = reduced(final, [[blocks[0][0]]], [far[0]])
    mixed = with_layout_constraint(mixed + laid(left, final, 0), Layout(major_to_minor=(0, 1)))
    mixed = lax.optimization_barrier(mixed)
    right = reduced(final, [[blocks[0][1][upper], blocks[0][1][lower]]], [far[1]])
    return mixed + laid(right, final, width // 2)


def solution(mesh):
    return jax.shard_map(
        steps,
        mesh=mesh,
        in_specs=(P("seq", "head"), P("seq", "head"), P("seq", "head"), P(), P("head", "seq")),
        out_specs=P("seq", "head"),
        check_vma=False,
    )
```

```python
import functools

import jax
import jax.numpy as jnp
import numpy as np
from jax import lax
from jax.experimental import pallas as pl
from jax.experimental.layout import Layout, with_layout_constraint
from jax.experimental.pallas import tpu as pltpu
from jax.sharding import PartitionSpec as P

HQ = 32
KV = 8
DH = 128
MOST = 2048
CALLS = 1


def attend_kernel(count, heads, column, first, lengths, q_ref, *refs):
    kv_refs = refs[: 2 * count]
    o_ref, k_buf, v_buf, m_ref, l_ref, acc_ref, sems = refs[2 * count + (not first) :]
    rows = q_ref.shape[0]
    factor = float(np.log2(np.e) / np.sqrt(DH))
    s, hops = lax.axis_index("seq"), count // 2 - 1
    q_first = s * rows

    def base_of(piece):
        hop = piece - hops - 1
        odd = s % 2
        along = s - 2 * piece
        across = jnp.where(odd == 1, s - 2 * hop - 1, s - 2 * hop + 1)
        valid = (across < s) & (hop <= hops - odd)
        return jnp.where(piece <= hops, along, jnp.where(valid, across, -(1 << 12))) * rows

    q_pos = q_first + lax.broadcasted_iota(jnp.int32, (1, rows), 1)

    def one_document(i, state):
        start, first_lo, last_lo, lo = state
        first_lo = jnp.where(start <= q_first, start, first_lo)
        last_lo = jnp.where(start < q_first + rows, start, last_lo)
        return start + lengths[i], first_lo, last_lo, jnp.where(start <= q_pos, start, lo)

    zero = jnp.int32(0)
    _, first_lo, last_lo, lo = lax.fori_loop(
        0, lengths.shape[0], one_document, (zero, zero, zero, jnp.zeros((1, rows), jnp.int32))
    )

    def copies(piece, at):
        for side, buf in enumerate((k_buf, v_buf)):
            yield pltpu.make_async_copy(
                kv_refs[side * count + at].at[:, column * DH : (column + 1) * DH],
                buf.at[piece],
                sems.at[side, piece],
            )

    for piece in range(count):

        @pl.when(first_lo < base_of(piece) + rows)
        def _():
            for copy in copies(piece, piece):
                copy.start()

    half = rows // 2

    def fold(piece, head, scores, first, columns, begin=0):
        top = jnp.max(scores, axis=0, keepdims=True)
        if not first:
            old = m_ref[head, :, columns]
            top = jnp.maximum(old, top)
        probs = jnp.exp2((scores - top) * factor)
        total = jnp.sum(probs, axis=0, keepdims=True)
        out = lax.dot_general(
            v_buf[piece, begin : begin + probs.shape[0]],
            probs.astype(jnp.bfloat16),
            (((0,), (0,)), ((), ())),
            preferred_element_type=jnp.float32,
        )
        if not first:
            fade = jnp.exp2((old - top) * factor)
            total = l_ref[head, :, columns] * fade + total
            out = acc_ref[head, :, columns] * fade + out
        m_ref[head, :, columns] = top
        l_ref[head, :, columns] = total
        acc_ref[head, :, columns] = out

    def scores_of(piece, head, count, columns, begin=0):
        return lax.dot_general(
            k_buf[piece, begin : begin + count],
            q_ref[columns, head * DH : (head + 1) * DH],
            (((1,), (1,)), ((), ())),
            preferred_element_type=jnp.float32,
        )

    for copy in copies(0, 0):
        copy.wait()
    for side in range(2):
        columns, deep = slice(side * half, (side + 1) * half), (side + 1) * half
        u = lax.broadcasted_iota(jnp.int32, (deep, half), 0)
        t = side * half + lax.broadcasted_iota(jnp.int32, (deep, half), 1)
        own = (u <= t) & (u >= lo[:, columns] - q_first)
        all_scores = [scores_of(0, head, deep, columns) for head in range(heads)]
        for head in range(heads):
            fold(0, head, jnp.where(own, all_scores[head], -1e30), True, columns)

    everything = slice(0, rows)

    @pl.loop(1, count)
    def _(piece):
        base = base_of(piece)
        needed = first_lo < base + rows

        @pl.when(needed)
        def _():
            for copy in copies(piece, 0):
                copy.wait()

        @pl.when(needed & (last_lo <= base))
        def _():
            all_scores = [scores_of(piece, head, rows, everything) for head in range(heads)]
            for head in range(heads):
                fold(piece, head, all_scores[head], False, everything)

        for begin, met in ((0, first_lo < base + half), (half, first_lo >= base + half)):

            @pl.when(needed & (last_lo > base) & met)
            def _():
                deep = rows - begin
                inside = lax.broadcasted_iota(jnp.int32, (deep, rows), 0) >= lo - (base + begin)
                all_scores = [scores_of(piece, head, deep, everything, begin) for head in range(heads)]
                for head in range(heads):
                    scores = jnp.where(inside, all_scores[head], -1e30)
                    fold(piece, head, scores, False, everything, begin)

    for head in range(heads):
        result = acc_ref[head] / l_ref[head]
        o_ref[:, head * DH : (head + 1) * DH] = result.T.astype(jnp.bfloat16)


def attend(lengths, queries, ks, vs, call, group, attn):
    rows, count, first = queries.shape[0], len(ks), attn is None
    anywhere = pl.BlockSpec(memory_space=pl.ANY)
    return pl.pallas_call(
        functools.partial(attend_kernel, count, group, call // CALLS, first),
        grid=(1,),
        out_shape=jax.ShapeDtypeStruct(queries.shape, jnp.bfloat16),
        in_specs=[
            pl.BlockSpec(memory_space=pltpu.SMEM),
            pl.BlockSpec((rows, group * DH), lambda i: (0, call)),
        ]
        + [anywhere] * (2 * count + (not first)),
        out_specs=pl.BlockSpec((rows, group * DH), lambda i: (0, call)),
        scratch_shapes=[
            pltpu.VMEM((count, rows, DH), jnp.bfloat16),
            pltpu.VMEM((count, rows, DH), jnp.bfloat16),
            pltpu.VMEM((group, 1, rows), jnp.float32),
            pltpu.VMEM((group, 1, rows), jnp.float32),
            pltpu.VMEM((group, DH, rows), jnp.float32),
            pltpu.SemaphoreType.DMA((2, count)),
        ],
        input_output_aliases={} if first else {2 + 2 * count: 0},
        cost_estimate=pl.CostEstimate(
            flops=4 * rows * rows * DH * group * count,
            bytes_accessed=4 * rows * DH * (group + count),
            transcendentals=rows * rows * group * count,
        ),
    )(lengths, queries, *ks, *vs, *([] if first else [attn]))


def steps(queries, keys, values, doc_lengths, out_weight):
    n, nh = lax.axis_size("seq"), lax.axis_size("head")
    rows = queries.shape[0]
    kv_local = keys.shape[1] // DH
    hops = -(-(-(-MOST // rows)) // 2)
    blocks_per_head = n // nh
    s, h = lax.axis_index("seq"), lax.axis_index("head")

    def spread(own):
        same, across = [own], []
        for hop in range(hops + 1):
            if hop > 0:
                up = [(i - 2, i) for i in range(2 * hop, n)]
                same.append(lax.ppermute(same[-1], "seq", up))
            pairs = [(i ^ 1, i) for i in range(2 * hop, n)]
            if hop == 0:
                pairs = [p for p in pairs if p[1] % 2 == 1]
            elif hop == hops:
                pairs = [p for p in pairs if p[1] % 2 == 0]
            across.append(lax.ppermute(same[-1], "seq", pairs))
        return same + across

    ks, vs = spread(keys), spread(values)

    order = list(range(0, n, 2)) + list(range(n - 1, 0, -2))
    place = {v: i for i, v in enumerate(order)}
    ahead = [(order[i], order[(i + 1) % n]) for i in range(n)]
    behind = [(b, a) for a, b in ahead]
    depth, width = out_weight.shape
    blocks = {0: [out_weight[:, : width // 2], out_weight[:, width // 2 :]]}
    forth, back = list(blocks[0]), list(blocks[0])
    for i in range(1, n // 2):
        for part in range(2):
            forth[part] = lax.ppermute(forth[part], "seq", ahead)
            back[part] = lax.ppermute(back[part], "seq", behind)
        blocks[-i], blocks[i] = list(forth), list(back)
    upper, lower = slice(0, depth // 2), slice(depth // 2, depth)
    far = [
        [lax.ppermute(forth[0], "seq", ahead)],
        [lax.ppermute(forth[1][upper], "seq", ahead), lax.ppermute(back[1][lower], "seq", behind)],
    ]

    pairs_of = [(i, i - n // 2) for i in range(1, n // 2)]
    pairs_of.sort(key=lambda p: max(p[0], -p[1]))
    pairs_of.append((0, n // 2))
    final = len(pairs_of) - 1

    def goal(i, shift):
        return order[(place[i] + shift) % n]

    def place_of(block):
        return jnp.where(block % 2 == 0, block // 2, n // 2 + (n - 1 - block) // 2)

    def head_of(shift):
        at = (place_of(s) + shift + n) % n
        return jnp.where(at < n // 2, 2 * at, 2 * (n - 1 - at) + 1) // blocks_per_head

    attn = None
    for call in range(kv_local * CALLS):
        attn = attend(doc_lengths, queries, ks, vs, call, HQ // KV // CALLS, attn)

    def times(chosen):
        at, total = 0, None
        for w in chosen:
            term = jnp.dot(attn[:, at : at + w.shape[0]], w, preferred_element_type=jnp.float32)
            total = term if total is None else total + term
            at += w.shape[0]
        return total.astype(jnp.bfloat16)

    def added(one, two):
        return (one.astype(jnp.float32) + two.astype(jnp.float32)).astype(jnp.bfloat16)

    def reduced(step, ones, twos):
        one_first = ((head_of(pairs_of[step][0]) ^ h) & 1) == 1
        swap = [(i * nh + j, i * nh + (j ^ 1)) for i in range(n) for j in range(nh)]
        sent = [times([jnp.where(one_first, a, b) for a, b in zip(x, y)]) for x, y in zip(ones, twos)]
        part = jnp.concatenate(sent, axis=1)
        arrived = lax.ppermute(part, ("seq", "head"), swap)
        kept = [times([jnp.where(one_first, b, a) for a, b in zip(x, y)]) for x, y in zip(ones, twos)]
        part = added(jnp.concatenate(kept, axis=1), arrived)
        bit = 2
        while bit < nh:
            pairs = []
            for i in range(n):
                for j in range(nh):
                    for shift in pairs_of[step]:
                        off = j ^ (goal(i, shift) // blocks_per_head)
                        if off & bit and not off & (bit - 1):
                            pairs.append((i * nh + j, i * nh + (j ^ bit)))
            arrived = lax.ppermute(part, ("seq", "head"), pairs)
            bit *= 2
            if bit < nh:
                part = added(part, arrived)
        return added(part, arrived)

    def laid(array, step, column):
        rest = blocks_per_head * width - array.shape[1]
        total = None
        for slot in range(blocks_per_head):
            ahead_by = (place_of(h * blocks_per_head + slot) - place_of(s) + n) % n
            here = (ahead_by == pairs_of[step][0] % n) | (ahead_by == pairs_of[step][1] % n)
            begin = slot * width + column
            term = jnp.where(here, array, jnp.zeros_like(array))
            term = lax.pad(term, jnp.bfloat16(0), ((0, 0, 0), (begin, rest - begin, 0)))
            total = term if total is None else total + term
        return total

    mixed = None
    for step, (one, two) in enumerate(pairs_of[:-1]):
        whole = reduced(step, [[w] for w in blocks[one]], [[w] for w in blocks[two]])
        part = laid(whole, step, 0)
        mixed = part if mixed is None else mixed + part
    left = reduced(final, [[blocks[0][0]]], [far[0]])
    mixed = with_layout_constraint(mixed + laid(left, final, 0), Layout(major_to_minor=(0, 1)))
    mixed = lax.optimization_barrier(mixed)
    right = reduced(final, [[blocks[0][1][upper], blocks[0][1][lower]]], [far[1]])
    return mixed + laid(right, final, width // 2)


def solution(mesh):
    return jax.shard_map(
        steps,
        mesh=mesh,
        in_specs=(P("seq", "head"), P("seq", "head"), P("seq", "head"), P(), P("head", "seq")),
        out_specs=P("seq", "head"),
        check_vma=False,
    )
```
